32 devices in a mesh: gx: 4 (over z), gy: 2 (over y), gz: 4 (over x, core).
Axes of the slice: x: 2, y: 2, z: 4, core: 2. Of those that a mesh axis runs over, the one named last changes fastest.
Arguments:
- strain: float32 [2, 4, 64, 32, 512], P(None, None, 'gx', 'gy', 'gz'), may hold values from -6 to 6
- cell_shell_index: int32 [64, 32, 512], P('gx', 'gy', 'gz'), may hold values from 0 to 255
- onset_step: int32 [256], replicated, may hold values from 0 to 1
Outputs:
- psi_four: float32 [2, 4, 64, 32, 512], P(None, None, 'gx', 'gy', 'gz')
- energy: float32 [4, 4, 256], P('gx', None, ('gy', 'gz'))
The draws below stay inside these ranges and needn't reach their ends.
All inputs are finite; a program needn't handle non-finite values.
Results may differ from the reference program's by a relative error of at most 0.00007.
Values sent between devices are 32-bit elements; how exact they have to be, the bound alone decides.
A program may use at most 64 MiB of HBM per device.

```python
import jax
import jax.numpy as jnp
from jax import lax

CX = 16
NT = 4
SHELLS = 256
NX = 64
NY = 32
NZ = 512
N_GX = 4


def set_ends(values, stream_key, smallest, largest):
    index_at = [jax.random.randint(jax.random.fold_in(stream_key, axis), (), 0, length) for axis, length in enumerate(values.shape)]
    main_axis = values.shape.index(max(values.shape))
    beside = index_at[:main_axis] + [(index_at[main_axis] + 1) % values.shape[main_axis]] + index_at[main_axis + 1:]
    return values.at[tuple(index_at)].set(smallest).at[tuple(beside)].set(largest)


def block_levels(own_key, dims, pieces, least, high):
    loudness, own = 1.0, jax.random.fold_in(own_key, 6)
    for position, shards_of in pieces:
        heights = jnp.exp(jax.random.uniform(jax.random.fold_in(own, position), (shards_of,), jnp.float32, least / len(pieces), high / len(pieces)))
        loudness = loudness * jnp.repeat(heights, dims[position] // shards_of).reshape([-1 if axis == position else 1 for axis in range(len(dims))])
    return loudness


def centred(rng, extent, spread, limit, split=(), held_as=jnp.bfloat16):
    array = jax.random.normal(rng, extent, jnp.float32) * spread
    if len(split) > 0:
        array = block_levels(rng, extent, split, -0.22, 0.18) * array
    return jnp.clip(array, min=-limit, max=limit).astype(held_as)


def setup_inputs(seed: int = 0) -> dict:
    keys = jax.random.split(jax.random.key(seed), 4)
    strain = centred(keys[0], (2, NT, NX, NY, NZ), 1.0, 6.0, ((2, 4), (3, 2), (4, 4)), jnp.float32)
    cell_shell_index = set_ends(jax.random.randint(keys[1], (NX, NY, NZ), 0, SHELLS), jax.random.fold_in(keys[1], 1), 0, SHELLS - 1).astype(jnp.int32)
    onset_step = set_ends(jax.random.randint(keys[2], (SHELLS,), 0, NT // 2), jax.random.fold_in(keys[2], 1), 0, (NT // 2) - 1).astype(jnp.int32)
    return dict(strain=strain, cell_shell_index=cell_shell_index, onset_step=onset_step)


first_coef = ((-2, 1.0), (-1, -8.0), (1, 8.0), (2, -1.0))
second_coef = ((-2, -1.0), (-1, 16.0), (0, -30.0), (1, 16.0), (2, -1.0))


def take_shifted(padded, off_x, off_y, off_z):
    len_x = padded.shape[2] - 4
    len_y = padded.shape[3] - 4
    len_z = padded.shape[4] - 4
    return padded[:, :, 2 + off_x:2 + off_x + len_x, 2 + off_y:2 + off_y + len_y, 2 + off_z:2 + off_z + len_z]


def reference(strain, cell_shell_index, onset_step):
    padded = jnp.pad(strain, ((0, 0), (0, 0), (2, 2), (2, 2), (2, 2)))
    second_x = sum(w * take_shifted(padded, k, 0, 0) for k, w in second_coef) / 12.0
    second_y = sum(w * take_shifted(padded, 0, k, 0) for k, w in second_coef) / 12.0
    second_z = sum(w * take_shifted(padded, 0, 0, k) for k, w in second_coef) / 12.0
    mixed_yz = sum(wa * wb * take_shifted(padded, 0, ka, kb) for ka, wa in first_coef for kb, wb in first_coef) / 144.0
    combo = second_x + second_y - second_z
    real_part = 0.5 * combo[0] - mixed_yz[1]
    imag_part = -0.5 * combo[1] - mixed_yz[0]
    psi_four = jnp.stack([real_part, imag_part])
    bondi_news = jnp.cumsum(psi_four, axis=1) * 0.25
    position_along_x = (jnp.arange(NX, dtype=jnp.float32) + 0.5) / NX - 0.5
    position_along_y = (jnp.arange(NY, dtype=jnp.float32) + 0.5) / NY - 0.5
    position_along_z = (jnp.arange(NZ, dtype=jnp.float32) + 0.5) / NZ - 0.5
    radius_squared = position_along_x[:, None, None] ** 2 + position_along_y[None, :, None] ** 2 + position_along_z[None, None, :] ** 2 + 0.05
    energy_flux = radius_squared[None] * (bondi_news[0] ** 2 + bondi_news[1] ** 2)
    flux_slabs = energy_flux.reshape(NT, N_GX, CX * NY * NZ)
    id_slabs = cell_shell_index.reshape(N_GX, CX * NY * NZ)

    def per_slab(slab):
        data = lax.dynamic_index_in_dim(flux_slabs, slab, 1, keepdims=False)
        ids = lax.dynamic_index_in_dim(id_slabs, slab, 0, keepdims=False)
        return jax.ops.segment_sum(data.T, ids, num_segments=SHELLS).T

    binned = lax.map(per_slab, jnp.arange(N_GX, dtype=jnp.int32))
    live = (jnp.arange(NT, dtype=jnp.int32)[:, None] >= onset_step[None, :]).astype(jnp.float32)
    binned = binned * live[None]
    scale = 0.25 * SHELLS / (NX * NY * NZ)
    energy = jnp.cumsum(jnp.cumsum(binned, axis=1), axis=0) * scale
    return psi_four, energy
```

```python
import functools

import jax
import jax.numpy as jnp
from jax import lax
from jax.experimental import pallas as pl
from jax.experimental.pallas import tpu as pltpu
from jax.sharding import PartitionSpec as P

MESH = pl.DeviceIdType.MESH
HI = 8


def step(sizes, strain, cells, onset, psi_out, energy, grid, index, psi, edges, ends, halo_z,
         rows_out, rows_low, rows_high, first_z, parts, acc, table, inbox, carry, slabs,
         load_sem, out_sem, send_x, recv_x, send_y, recv_y, send_z, recv_z,
         send_bin, recv_bin, send_acc, recv_acc):
    ngx, ngy, ngz, steps, cx, cy, cz, shells = sizes
    fields = 2 * steps
    n_lo = shells // HI
    peers = ngy * ngz
    own = shells // peers
    gx, gy, gz = lax.axis_index("gx"), lax.axis_index("gy"), lax.axis_index("gz")
    rank = gy * ngz + gz

    load = pltpu.make_async_copy(strain, grid.at[:, pl.ds(2, cx), pl.ds(8, cy), :], load_sem.at[0])
    load.start()
    load_index = pltpu.make_async_copy(cells, index, load_sem.at[1])
    load_index.start()

    barrier = pltpu.get_barrier_semaphore()

    def greet_slab(k, _):
        q = lax.rem(rank + k, peers)
        pl.semaphore_signal(barrier, inc=1, device_id=(gx, q // ngz, lax.rem(q, ngz)), device_id_type=MESH)
        return 0

    def greet_line(k, _):
        pl.semaphore_signal(barrier, inc=1, device_id=(lax.rem(gx + k, ngx), gy, gz), device_id_type=MESH)
        return 0

    lax.fori_loop(1, ngx, greet_line, 0)
    lax.fori_loop(1, peers, greet_slab, 0)
    load.wait()

    lane = lax.broadcasted_iota(jnp.int32, (8, cz), 1)
    row = lax.broadcasted_iota(jnp.int32, (8, cz), 0)
    slot_of_lane = lane // 4

    for f in range(fields):
        packed = jnp.zeros((8, cz), jnp.float32)
        for x in range(cx):
            rows_out[0, pl.ds(f * 2 * cx + 2 * x, 2), :] = grid[f, x + 2, pl.ds(8, 2), :]
            rows_out[1, pl.ds(f * 2 * cx + 2 * x, 2), :] = grid[f, x + 2, pl.ds(6 + cy, 2), :]
            for half in range(2):
                slot = 2 * x + half
                moved = pltpu.roll(grid[f, x + 2, pl.ds(8 + 8 * half, 8), :], (2 + 4 * slot) % cz, 1)
                packed = jnp.where(slot_of_lane == slot, moved, packed)
        edges[f] = packed

    pl.semaphore_wait(barrier, peers - 1 + ngx - 1)

    def x_copy(side):
        there = gx + 1 if side == 0 else gx - 1
        return pltpu.make_async_remote_copy(
            src_ref=grid.at[:, pl.ds(cx if side == 0 else 2, 2), pl.ds(8, cy), :],
            dst_ref=grid.at[:, pl.ds(0 if side == 0 else cx + 2, 2), pl.ds(8, cy), :],
            send_sem=send_x.at[side], recv_sem=recv_x.at[side],
            device_id=(there, gy, gz), device_id_type=MESH)

    def y_copy(side):
        there = gy + 1 if side == 0 else gy - 1
        return pltpu.make_async_remote_copy(
            src_ref=rows_out.at[1 - side],
            dst_ref=(rows_low.at[pl.ds(8, fields * 2 * cx), :] if side == 0
                     else rows_high.at[pl.ds(0, fields * 2 * cx), :]),
            send_sem=send_y.at[side], recv_sem=recv_y.at[side],
            device_id=(gx, there, gz), device_id_type=MESH)

    def z_copy(side, dy):
        there = gz + 1 if side == 0 else gz - 1
        return pltpu.make_async_remote_copy(
            src_ref=edges, dst_ref=ends.at[side, 1 - dy],
            send_sem=send_z.at[side, 1 - dy], recv_sem=recv_z.at[side, 1 - dy],
            device_id=(gx, gy + dy, there), device_id_type=MESH)

    sends = ([gz < ngz - 1, gz > 0], [gy < ngy - 1, gy > 0], [gx < ngx - 1, gx > 0])
    gets = ([gz > 0, gz < ngz - 1], [gy > 0, gy < ngy - 1], [gx > 0, gx < ngx - 1])
    near = {-1: gy > 0, 0: gy >= 0, 1: gy < ngy - 1}

    for side in range(2):
        for dy in (0, -1, 1):
            @pl.when(jnp.logical_and(sends[0][side], near[dy]))
            def _(side=side, dy=dy):
                z_copy(side, dy).start()
    for side in range(2):
        @pl.when(sends[1][side])
        def _(side=side):
            y_copy(side).start()
    for side in range(2):
        @pl.when(sends[2][side])
        def _(side=side):
            x_copy(side).start()

    for side in range(2):
        for dy in (-1, 0, 1):
            @pl.when(jnp.logical_not(jnp.logical_and(gets[0][side], near[dy])))
            def _(side=side, dy=dy):
                ends[side, 1 + dy] = jnp.zeros(ends.shape[2:], jnp.float32)

        @pl.when(jnp.logical_not(gets[2][side]))
        def _(side=side):
            grid[:, pl.ds(0 if side == 0 else cx + 2, 2), pl.ds(8, cy), :] = jnp.zeros(
                (fields, 2, cy, cz), jnp.float32)

    @pl.when(jnp.logical_not(gets[1][0]))
    def _():
        rows_low[...] = jnp.zeros(rows_low.shape, jnp.float32)

    @pl.when(jnp.logical_not(gets[1][1]))
    def _():
        rows_high[...] = jnp.zeros(rows_high.shape, jnp.float32)

    acc[...] = jnp.zeros(acc.shape, jnp.float32)
    table[...] = jnp.zeros(table.shape, jnp.float32)
    load_index.wait()

    for side in range(2):
        for dy in (0, -1, 1):
            @pl.when(jnp.logical_and(gets[0][side], near[dy]))
            def _(side=side, dy=dy):
                z_copy(side, -dy).wait_recv()

    from_left = lax.rem(lane, 4) < 2
    for f in range(fields):
        halo_z[0, f] = jnp.where(from_left, ends[0, 1, f], ends[1, 1, f])
        low = jnp.where(from_left, ends[0, 0, f], ends[1, 0, f])
        high = jnp.where(from_left, ends[0, 2, f], ends[1, 2, f])
        halo_z[1, f] = jnp.where(row < 4, pltpu.roll(high, 4, 1), low)

    for side in range(2):
        @pl.when(gets[1][side])
        def _(side=side):
            y_copy(side).wait_recv()

    wide = lax.broadcasted_iota(jnp.int32, (cy, cz), 0)
    far = lax.broadcasted_iota(jnp.int32, (cy, cz), 1)
    uy = ((gy * cy + wide).astype(jnp.float32) + 0.5) / (cy * ngy) - 0.5
    uz = ((gz * cz + far).astype(jnp.float32) + 0.5) / (cz * ngz) - 0.5
    rsq_yz = uy * uy + uz * uz + 0.05
    low_label = lax.broadcasted_iota(jnp.int32, (n_lo, cz), 0)
    head, tail = lane < 2, lane >= cz - 2

    def along(cell, halo, shift):
        ring = pltpu.roll(halo, shift, 1)
        m2 = pltpu.roll(jnp.where(tail, ring, cell), 2, 1)
        m1 = pltpu.roll(jnp.where(lane == cz - 1, ring, cell), 1, 1)
        p1 = pltpu.roll(jnp.where(lane == 0, ring, cell), cz - 1, 1)
        p2 = pltpu.roll(jnp.where(head, ring, cell), cz - 2, 1)
        return m2, m1, p1, p2

    def plane(i, _):
        x = lax.rem(i + 2, cx)

        @pl.when(i == cx - 4)
        def _():
            for side in range(2):
                @pl.when(gets[2][side])
                def _(side=side):
                    x_copy(side).wait_recv()

        shift0 = lax.rem(2 * cz - 2 - 8 * x, cz)
        shift1 = lax.rem(2 * cz - 6 - 8 * x, cz)
        combo, mixed = [], []
        for f in range(fields):
            base = f * 2 * cx + 2 * x
            outside = jnp.where(row < 4, rows_high[pl.ds(base, 8), :], rows_low[pl.ds(base + 2, 8), :])
            grid[f, x + 2, pl.ds(0, 8), :] = outside
            grid[f, x + 2, pl.ds(8 + cy, 8), :] = outside
            m2, m1, p1, p2 = along(outside, halo_z[1, f], shift1)
            d = 8.0 * (p1 - m1) - (p2 - m2)
            first_z[f, pl.ds(0, 8), :] = d
            first_z[f, pl.ds(8 + cy, 8), :] = d
            seconds = []
            for half in range(2):
                cell = grid[f, x + 2, pl.ds(8 + 8 * half, 8), :]
                m2, m1, p1, p2 = along(cell, halo_z[0, f], shift1 if half else shift0)
                first_z[f, pl.ds(8 + 8 * half, 8), :] = 8.0 * (p1 - m1) - (p2 - m2)
                seconds.append(16.0 * (p1 + m1) - (p2 + m2))
            center = grid[f, x + 2, pl.ds(8, cy), :]
            near_xy = (grid[f, x + 1, pl.ds(8, cy), :] + grid[f, x + 3, pl.ds(8, cy), :]
                       + grid[f, x + 2, pl.ds(7, cy), :] + grid[f, x + 2, pl.ds(9, cy), :])
            far_xy = (grid[f, x, pl.ds(8, cy), :] + grid[f, x + 4, pl.ds(8, cy), :]
                      + grid[f, x + 2, pl.ds(6, cy), :] + grid[f, x + 2, pl.ds(10, cy), :])
            combo.append(16.0 * near_xy - far_xy - 30.0 * center - jnp.concatenate(seconds, 0))
            mixed.append(8.0 * (first_z[f, pl.ds(9, cy), :] - first_z[f, pl.ds(7, cy), :])
                         - (first_z[f, pl.ds(10, cy), :] - first_z[f, pl.ds(6, cy), :]))
        ux = ((gx * cx + x).astype(jnp.float32) + 0.5) * (1.0 / (cx * ngx)) - 0.5
        rsq = (rsq_yz + ux * ux) * 0.0625
        news_re = jnp.zeros((cy, cz), jnp.float32)
        news_im = jnp.zeros((cy, cz), jnp.float32)
        for t in range(steps):
            re = combo[t] * (1.0 / 24.0) - mixed[steps + t] * (1.0 / 144.0)
            im = combo[steps + t] * (-1.0 / 24.0) - mixed[t] * (1.0 / 144.0)
            psi[t, x] = re
            psi[steps + t, x] = im
            news_re, news_im = news_re + re, news_im + im
            flux = rsq * (news_re * news_re + news_im * news_im)
            coarse = flux.astype(jnp.bfloat16).astype(jnp.float32)
            parts[2 * t] = coarse
            parts[2 * t + 1] = flux - coarse
        pltpu.make_async_copy(psi.at[:, x], psi_out.at[:, x], out_sem.at[x]).start()

        total = acc[...]
        group = 4
        for y0 in range(0, cy, group):
            left, right = [], []
            hit = []
            for y in range(y0, y0 + group):
                shell = index[x, pl.ds(y, 1), :]
                high = shell // n_lo
                low = shell - high * n_lo
                hit.append(jnp.broadcast_to(high, (HI, cz)) == row)
                right.append(jnp.where(jnp.broadcast_to(low, (n_lo, cz)) == low_label, 1.0, 0.0))
            for p in range(2 * steps):
                left.append(jnp.concatenate(
                    [jnp.where(hit[k], jnp.broadcast_to(parts[p, pl.ds(y0 + k, 1), :], (HI, cz)), 0.0)
                     for k in range(group)], 1))
            total = total + lax.dot_general(
                jnp.concatenate(left, 0).astype(jnp.bfloat16),
                jnp.concatenate(right, 1).astype(jnp.bfloat16),
                (((1,), (1,)), ((), ())), preferred_element_type=jnp.float32)
        acc[...] = total
        return 0

    lax.fori_loop(0, cx, plane, 0)

    for t in range(steps):
        both = acc[pl.ds(16 * t, 8), :] + acc[pl.ds(16 * t + 8, 8), :]
        for h in range(HI):
            table[h, pl.ds(t, 1), pl.ds(0, n_lo)] = both[h:h + 1, :]

    spread = peers // HI

    def bin_copy(k):
        q = lax.rem(rank + k, peers)
        return pltpu.make_async_remote_copy(
            src_ref=table.at[q // spread], dst_ref=inbox.at[rank],
            send_sem=send_bin.at[k], recv_sem=recv_bin.at[rank],
            device_id=(gx, q // ngz, lax.rem(q, ngz)), device_id_type=MESH)

    def bin_arrival(k):
        q = lax.rem(rank + k, peers)
        return pltpu.make_async_remote_copy(
            src_ref=table.at[0], dst_ref=inbox.at[q],
            send_sem=send_bin.at[k], recv_sem=recv_bin.at[q],
            device_id=(gx, q // ngz, lax.rem(q, ngz)), device_id_type=MESH)

    def send_one(k, _):
        bin_copy(k).start()
        return 0

    lax.fori_loop(1, peers, send_one, 0)

    def take_one(k, total):
        bin_arrival(k).wait_recv()
        return total + inbox[lax.rem(rank + k, peers)]

    total = lax.fori_loop(1, peers, take_one, table[rank // spread])
    first = rank * own
    labels = jnp.zeros((8, 128), jnp.int32)
    for block in range(shells // 128):
        piece = jnp.broadcast_to(onset[:, pl.ds(block * 128, 128)], (8, 128))
        labels = jnp.where(first // 128 == block, piece, labels)
    labels = pltpu.roll(labels, lax.rem(128 - lax.rem(first, 128), 128), 1)
    total = pltpu.roll(total, lax.rem(128 - lax.rem(rank, spread) * own, 128), 1)
    total = jnp.where(row >= labels, total, 0.0)
    scale = 0.25 * shells / (cx * ngx * cy * ngy * cz * ngz)
    running = jnp.zeros((1, 128), jnp.float32)
    sums = []
    for t in range(steps):
        running = running + total[t:t + 1, :]
        sums.append(running * scale)
    sums.append(jnp.zeros((8 - steps, 128), jnp.float32))
    mine = jnp.concatenate(sums, 0)
    carry[...] = mine

    def line_copy(there):
        return pltpu.make_async_remote_copy(
            src_ref=carry, dst_ref=slabs.at[gx],
            send_sem=send_acc.at[there], recv_sem=recv_acc.at[gx],
            device_id=(there, gy, gz), device_id_type=MESH)

    def line_arrival(h):
        return pltpu.make_async_remote_copy(
            src_ref=carry, dst_ref=slabs.at[h],
            send_sem=send_acc.at[h], recv_sem=recv_acc.at[h],
            device_id=(h, gy, gz), device_id_type=MESH)

    def send_line(k, _):
        line_copy(gx + k).start()
        return 0

    lax.fori_loop(1, ngx - gx, send_line, 0)

    def take_line(h, total):
        line_arrival(h).wait_recv()
        return total + slabs[h]

    energy[...] = lax.fori_loop(0, gx, take_line, mine)[:steps, :own]

    def end_out(x, _):
        pltpu.make_async_copy(psi.at[:, x], psi_out.at[:, x], out_sem.at[x]).wait()
        return 0

    lax.fori_loop(0, cx, end_out, 0)

    for side in range(2):
        for dy in (0, -1, 1):
            @pl.when(jnp.logical_and(sends[0][side], near[dy]))
            def _(side=side, dy=dy):
                z_copy(side, dy).wait_send()

        @pl.when(sends[1][side])
        def _(side=side):
            y_copy(side).wait_send()

        @pl.when(sends[2][side])
        def _(side=side):
            x_copy(side).wait_send()

    def end_one(k, _):
        bin_copy(k).wait_send()
        return 0

    lax.fori_loop(1, peers, end_one, 0)

    def end_line(k, _):
        line_copy(gx + k).wait_send()
        return 0

    lax.fori_loop(1, ngx - gx, end_line, 0)


def body(strain, cell_shell_index, onset_step):
    comps, steps, cx, cy, cz = strain.shape
    shells = onset_step.shape[0]
    ngx, ngy, ngz = lax.axis_size("gx"), lax.axis_size("gy"), lax.axis_size("gz")
    peers = ngy * ngz
    own = shells // peers
    fields = comps * steps
    n_lo = shells // HI
    f32 = jnp.float32
    dma = pltpu.SemaphoreType.DMA
    sizes = (ngx, ngy, ngz, steps, cx, cy, cz, shells)
    anywhere = pl.BlockSpec(memory_space=pl.ANY)
    vmem = pl.BlockSpec(memory_space=pltpu.VMEM)
    psi, energy = pl.pallas_call(
        functools.partial(step, sizes),
        out_shape=(
            jax.ShapeDtypeStruct((fields, cx, cy, cz), f32),
            jax.ShapeDtypeStruct((steps, own), f32),
        ),
        in_specs=[anywhere, anywhere, vmem],
        out_specs=(anywhere, vmem),
        scratch_shapes=[
            pltpu.VMEM((fields, cx + 4, cy + 16, cz), f32),
            pltpu.VMEM((cx, cy, cz), jnp.int32),
            pltpu.VMEM((fields, cx, cy, cz), f32),
            pltpu.VMEM((fields, 8, cz), f32),
            pltpu.VMEM((2, 3, fields, 8, cz), f32),
            pltpu.VMEM((2, fields, 8, cz), f32),
            pltpu.VMEM((2, fields * 2 * cx, cz), f32),
            pltpu.VMEM((fields * 2 * cx + 8, cz), f32),
            pltpu.VMEM((fields * 2 * cx + 8, cz), f32),
            pltpu.VMEM((fields, cy + 16, cz), f32),
            pltpu.VMEM((2 * steps, cy, cz), f32),
            pltpu.VMEM((2 * steps * HI, n_lo), f32),
            pltpu.VMEM((HI, 8, 128), f32),
            pltpu.VMEM((peers, 8, 128), f32),
            pltpu.VMEM((8, 128), f32),
            pltpu.VMEM((ngx, 8, 128), f32),
            dma((2,)), dma((cx,)),
            dma((2,)), dma((2,)), dma((2,)), dma((2,)), dma((2, 3)), dma((2, 3)),
            dma((peers,)), dma((peers,)), dma((ngx,)), dma((ngx,)),
        ],
        compiler_params=pltpu.CompilerParams(
            collective_id=0, has_side_effects=True, vmem_limit_bytes=32 * 1024 * 1024),
    )(strain.reshape(fields, cx, cy, cz), cell_shell_index, onset_step.reshape(1, shells))
    return psi.reshape(strain.shape), energy[None]


def solution(mesh):
    placed = (P(None, None, "gx", "gy", "gz"), P("gx", "gy", "gz"), P())
    return jax.shard_map(
        body,
        mesh=mesh,
        in_specs=placed,
        out_specs=(P(None, None, "gx", "gy", "gz"), P("gx", None, ("gy", "gz"))),
        check_vma=False,
    )
```

```python
import functools

import jax
import jax.numpy as jnp
from jax import lax
from jax.experimental import pallas as pl
from jax.experimental.pallas import tpu as pltpu
from jax.sharding import PartitionSpec as P

MESH = pl.DeviceIdType.MESH
HI = 8


def step(sizes, strain, cells, onset, psi_out, energy, grid, index, psi, edges, ends, halo_z, corners, corner_in, slope_low, slope_high,
         rows_out, rows_low, rows_high, first_z, parts, acc, table, inbox, carry, slabs,
         load_sem, out_sem, send_x, recv_x, send_y, recv_y, send_z, recv_z,
         send_bin, recv_bin, send_acc, recv_acc):
    ngx, ngy, ngz, steps, cx, cy, cz, shells = sizes
    fields = 2 * steps
    n_lo = shells // HI
    peers = ngy * ngz
    own = shells // peers
    gx, gy, gz = lax.axis_index("gx"), lax.axis_index("gy"), lax.axis_index("gz")
    rank = gy * ngz + gz

    load = pltpu.make_async_copy(strain, grid.at[:, pl.ds(2, cx), pl.ds(8, cy), :], load_sem.at[0])
    load.start()
    load_index = pltpu.make_async_copy(cells, index, load_sem.at[1])
    load_index.start()

    barrier = pltpu.get_barrier_semaphore()

    def greet_slab(k, _):
        q = lax.rem(rank + k, peers)
        pl.semaphore_signal(barrier, inc=1, device_id=(gx, q // ngz, lax.rem(q, ngz)), device_id_type=MESH)
        return 0

    def greet_line(k, _):
        pl.semaphore_signal(barrier, inc=1, device_id=(lax.rem(gx + k, ngx), gy, gz), device_id_type=MESH)
        return 0

    lax.fori_loop(1, ngx, greet_line, 0)
    lax.fori_loop(1, peers, greet_slab, 0)
    load.wait()

    lane = lax.broadcasted_iota(jnp.int32, (8, cz), 1)
    row = lax.broadcasted_iota(jnp.int32, (8, cz), 0)
    slot_of_lane = lane // 4

    for f in range(fields):
        packed = jnp.zeros((8, cz), jnp.float32)
        for x in range(cx):
            rows_out[0, pl.ds(f * 2 * cx + 2 * x, 2), :] = grid[f, x + 2, pl.ds(8, 2), :]
            rows_out[1, pl.ds(f * 2 * cx + 2 * x, 2), :] = grid[f, x + 2, pl.ds(6 + cy, 2), :]
            for half in range(2):
                slot = 2 * x + half
                moved = pltpu.roll(grid[f, x + 2, pl.ds(8 + 8 * half, 8), :], (2 + 4 * slot) % cz, 1)
                packed = jnp.where(slot_of_lane == slot, moved, packed)
        edges[f] = packed

    for side in range(2):
        packed = jnp.zeros((8, cz), jnp.float32)
        for slot in range(fields * cx // 4):
            moved = pltpu.roll(rows_out[side, pl.ds(8 * slot, 8), :], (2 + 4 * slot) % cz, 1)
            packed = jnp.where(slot_of_lane == slot, moved, packed)
        corners[side] = packed

    pl.semaphore_wait(barrier, peers - 1 + ngx - 1)

    def x_copy(side):
        there = gx + 1 if side == 0 else gx - 1
        return pltpu.make_async_remote_copy(
            src_ref=grid.at[:, pl.ds(cx if side == 0 else 2, 2), pl.ds(8, cy), :],
            dst_ref=grid.at[:, pl.ds(0 if side == 0 else cx + 2, 2), pl.ds(8, cy), :],
            send_sem=send_x.at[side], recv_sem=recv_x.at[side],
            device_id=(there, gy, gz), device_id_type=MESH)

    def y_copy(side):
        there = gy + 1 if side == 0 else gy - 1
        return pltpu.make_async_remote_copy(
            src_ref=rows_out.at[1 - side],
            dst_ref=(rows_low.at[pl.ds(8, fields * 2 * cx), :] if side == 0
                     else rows_high.at[pl.ds(0, fields * 2 * cx), :]),
            send_sem=send_y.at[side], recv_sem=recv_y.at[side],
            device_id=(gx, there, gz), device_id_type=MESH)

    def z_copy(side, dy):
        there = gz + 1 if side == 0 else gz - 1
        return pltpu.make_async_remote_copy(
            src_ref=edges if dy == 0 else corners.at[0 if dy < 0 else 1],
            dst_ref=ends.at[side] if dy == 0 else corner_in.at[side, 0 if dy > 0 else 1],
            send_sem=send_z.at[side, 1 - dy], recv_sem=recv_z.at[side, 1 - dy],
            device_id=(gx, gy + dy, there), device_id_type=MESH)

    sends = ([gz < ngz - 1, gz > 0], [gy < ngy - 1, gy > 0], [gx < ngx - 1, gx > 0])
    gets = ([gz > 0, gz < ngz - 1], [gy > 0, gy < ngy - 1], [gx > 0, gx < ngx - 1])
    near = {-1: gy > 0, 0: gy >= 0, 1: gy < ngy - 1}

    for side in range(2):
        for dy in (0, -1, 1):
            @pl.when(jnp.logical_and(sends[0][side], near[dy]))
            def _(side=side, dy=dy):
                z_copy(side, dy).start()
    for side in range(2):
        @pl.when(sends[1][side])
        def _(side=side):
            y_copy(side).start()
    for side in range(2):
        @pl.when(sends[2][side])
        def _(side=side):
            x_copy(side).start()

    for side in range(2):
        for dy in (-1, 0, 1):
            @pl.when(jnp.logical_not(jnp.logical_and(gets[0][side], near[dy])))
            def _(side=side, dy=dy):
                if dy == 0:
                    ends[side] = jnp.zeros(ends.shape[1:], jnp.float32)
                else:
                    corner_in[side, 0 if dy < 0 else 1] = jnp.zeros((8, cz), jnp.float32)

        @pl.when(jnp.logical_not(gets[2][side]))
        def _(side=side):
            grid[:, pl.ds(0 if side == 0 else cx + 2, 2), pl.ds(8, cy), :] = jnp.zeros(
                (fields, 2, cy, cz), jnp.float32)

    @pl.when(jnp.logical_not(gets[1][0]))
    def _():
        rows_low[...] = jnp.zeros(rows_low.shape, jnp.float32)

    @pl.when(jnp.logical_not(gets[1][1]))
    def _():
        rows_high[...] = jnp.zeros(rows_high.shape, jnp.float32)

    acc[...] = jnp.zeros(acc.shape, jnp.float32)
    table[...] = jnp.zeros(table.shape, jnp.float32)
    load_index.wait()

    for side in range(2):
        for dy in (0, -1, 1):
            @pl.when(jnp.logical_and(gets[0][side], near[dy]))
            def _(side=side, dy=dy):
                z_copy(side, -dy).wait_recv()

    from_left = lax.rem(lane, 4) < 2
    for f in range(fields):
        halo_z[f] = jnp.where(from_left, ends[0, f], ends[1, f])

    for side in range(2):
        @pl.when(gets[1][side])
        def _(side=side):
            y_copy(side).wait_recv()

    wide = lax.broadcasted_iota(jnp.int32, (cy, cz), 0)
    far = lax.broadcasted_iota(jnp.int32, (cy, cz), 1)
    uy = ((gy * cy + wide).astype(jnp.float32) + 0.5) / (cy * ngy) - 0.5
    uz = ((gz * cz + far).astype(jnp.float32) + 0.5) / (cz * ngz) - 0.5
    rsq_yz = uy * uy + uz * uz + 0.05
    low_label = lax.broadcasted_iota(jnp.int32, (n_lo, cz), 0)
    head, tail = lane < 2, lane >= cz - 2

    def along(cell, halo, shift):
        ring = pltpu.roll(halo, shift, 1)
        m2 = pltpu.roll(jnp.where(tail, ring, cell), 2, 1)
        m1 = pltpu.roll(jnp.where(lane == cz - 1, ring, cell), 1, 1)
        p1 = pltpu.roll(jnp.where(lane == 0, ring, cell), cz - 1, 1)
        p2 = pltpu.roll(jnp.where(head, ring, cell), cz - 2, 1)
        return m2, m1, p1, p2

    for end, (rows, first, slope) in enumerate(((rows_low, 8, slope_low), (rows_high, 0, slope_high))):
        @pl.when(gets[1][end])
        def _(end=end, rows=rows, first=first, slope=slope):
            ring = jnp.where(from_left, corner_in[0, end], corner_in[1, end])
            for slot in range(fields * cx // 4):
                m2, m1, p1, p2 = along(rows[pl.ds(first + 8 * slot, 8), :], ring, (2 * cz - 2 - 4 * slot) % cz)
                slope[pl.ds(first + 8 * slot, 8), :] = 8.0 * (p1 - m1) - (p2 - m2)

        @pl.when(jnp.logical_not(gets[1][end]))
        def _(slope=slope):
            slope[...] = jnp.zeros(slope.shape, jnp.float32)


    def plane(i, _):
        x = lax.rem(i + 2, cx)

        @pl.when(i == cx - 4)
        def _():
            for side in range(2):
                @pl.when(gets[2][side])
                def _(side=side):
                    x_copy(side).wait_recv()

        shift0 = lax.rem(2 * cz - 2 - 8 * x, cz)
        shift1 = lax.rem(2 * cz - 6 - 8 * x, cz)
        combo, mixed = [], []
        for f in range(fields):
            base = f * 2 * cx + 2 * x
            outside = jnp.where(row < 4, rows_high[pl.ds(base, 8), :], rows_low[pl.ds(base + 2, 8), :])
            grid[f, x + 2, pl.ds(0, 8), :] = outside
            grid[f, x + 2, pl.ds(8 + cy, 8), :] = outside
            d = jnp.where(row < 4, slope_high[pl.ds(base, 8), :], slope_low[pl.ds(base + 2, 8), :])
            first_z[f, pl.ds(0, 8), :] = d
            first_z[f, pl.ds(8 + cy, 8), :] = d
            seconds = []
            for half in range(2):
                cell = grid[f, x + 2, pl.ds(8 + 8 * half, 8), :]
                m2, m1, p1, p2 = along(cell, halo_z[f], shift1 if half else shift0)
                first_z[f, pl.ds(8 + 8 * half, 8), :] = 8.0 * (p1 - m1) - (p2 - m2)
                seconds.append(16.0 * (p1 + m1) - (p2 + m2))
            center = grid[f, x + 2, pl.ds(8, cy), :]
            near_xy = (grid[f, x + 1, pl.ds(8, cy), :] + grid[f, x + 3, pl.ds(8, cy), :]
                       + grid[f, x + 2, pl.ds(7, cy), :] + grid[f, x + 2, pl.ds(9, cy), :])
            far_xy = (grid[f, x, pl.ds(8, cy), :] + grid[f, x + 4, pl.ds(8, cy), :]
                      + grid[f, x + 2, pl.ds(6, cy), :] + grid[f, x + 2, pl.ds(10, cy), :])
            combo.append(16.0 * near_xy - far_xy - 30.0 * center - jnp.concatenate(seconds, 0))
            mixed.append(8.0 * (first_z[f, pl.ds(9, cy), :] - first_z[f, pl.ds(7, cy), :])
                         - (first_z[f, pl.ds(10, cy), :] - first_z[f, pl.ds(6, cy), :]))
        ux = ((gx * cx + x).astype(jnp.float32) + 0.5) * (1.0 / (cx * ngx)) - 0.5
        rsq = (rsq_yz + ux * ux) * 0.0625
        news_re = jnp.zeros((cy, cz), jnp.float32)
        news_im = jnp.zeros((cy, cz), jnp.float32)
        for t in range(steps):
            re = combo[t] * (1.0 / 24.0) - mixed[steps + t] * (1.0 / 144.0)
            im = combo[steps + t] * (-1.0 / 24.0) - mixed[t] * (1.0 / 144.0)
            psi[t, x] = re
            psi[steps + t, x] = im
            news_re, news_im = news_re + re, news_im + im
            flux = rsq * (news_re * news_re + news_im * news_im)
            coarse = flux.astype(jnp.bfloat16).astype(jnp.float32)
            parts[2 * t] = coarse
            parts[2 * t + 1] = flux - coarse
        pltpu.make_async_copy(psi.at[:, x], psi_out.at[:, x], out_sem.at[x]).start()

        total = acc[...]
        group = 4
        for y0 in range(0, cy, group):
            left, right = [], []
            hit = []
            for y in range(y0, y0 + group):
                shell = index[x, pl.ds(y, 1), :]
                high = shell // n_lo
                low = shell - high * n_lo
                hit.append(jnp.broadcast_to(high, (HI, cz)) == row)
                right.append(jnp.where(jnp.broadcast_to(low, (n_lo, cz)) == low_label, 1.0, 0.0))
            for p in range(2 * steps):
                left.append(jnp.concatenate(
                    [jnp.where(hit[k], jnp.broadcast_to(parts[p, pl.ds(y0 + k, 1), :], (HI, cz)), 0.0)
                     for k in range(group)], 1))
            total = total + lax.dot_general(
                jnp.concatenate(left, 0).astype(jnp.bfloat16),
                jnp.concatenate(right, 1).astype(jnp.bfloat16),
                (((1,), (1,)), ((), ())), preferred_element_type=jnp.float32)
        acc[...] = total
        return 0

    lax.fori_loop(0, cx, plane, 0)

    for t in range(steps):
        both = acc[pl.ds(16 * t, 8), :] + acc[pl.ds(16 * t + 8, 8), :]
        for h in range(HI):
            table[h, pl.ds(t, 1), pl.ds(0, n_lo)] = both[h:h + 1, :]

    spread = peers // HI

    def bin_copy(k):
        q = lax.rem(rank + k, peers)
        return pltpu.make_async_remote_copy(
            src_ref=table.at[q // spread], dst_ref=inbox.at[rank],
            send_sem=send_bin.at[k], recv_sem=recv_bin.at[rank],
            device_id=(gx, q // ngz, lax.rem(q, ngz)), device_id_type=MESH)

    def bin_arrival(k):
        q = lax.rem(rank + k, peers)
        return pltpu.make_async_remote_copy(
            src_ref=table.at[0], dst_ref=inbox.at[q],
            send_sem=send_bin.at[k], recv_sem=recv_bin.at[q],
            device_id=(gx, q // ngz, lax.rem(q, ngz)), device_id_type=MESH)

    def send_one(k, _):
        bin_copy(k).start()
        return 0

    lax.fori_loop(1, peers, send_one, 0)

    def take_one(k, total):
        bin_arrival(k).wait_recv()
        return total + inbox[lax.rem(rank + k, peers)]

    total = lax.fori_loop(1, peers, take_one, table[rank // spread])
    first = rank * own
    labels = jnp.zeros((8, 128), jnp.int32)
    for block in range(shells // 128):
        piece = jnp.broadcast_to(onset[:, pl.ds(block * 128, 128)], (8, 128))
        labels = jnp.where(first // 128 == block, piece, labels)
    labels = pltpu.roll(labels, lax.rem(128 - lax.rem(first, 128), 128), 1)
    total = pltpu.roll(total, lax.rem(128 - lax.rem(rank, spread) * own, 128), 1)
    total = jnp.where(row >= labels, total, 0.0)
    scale = 0.25 * shells / (cx * ngx * cy * ngy * cz * ngz)
    running = jnp.zeros((1, 128), jnp.float32)
    sums = []
    for t in range(steps):
        running = running + total[t:t + 1, :]
        sums.append(running * scale)
    sums.append(jnp.zeros((8 - steps, 128), jnp.float32))
    mine = jnp.concatenate(sums, 0)
    carry[...] = mine

    def line_copy(there):
        return pltpu.make_async_remote_copy(
            src_ref=carry, dst_ref=slabs.at[gx],
            send_sem=send_acc.at[there], recv_sem=recv_acc.at[gx],
            device_id=(there, gy, gz), device_id_type=MESH)

    def line_arrival(h):
        return pltpu.make_async_remote_copy(
            src_ref=carry, dst_ref=slabs.at[h],
            send_sem=send_acc.at[h], recv_sem=recv_acc.at[h],
            device_id=(h, gy, gz), device_id_type=MESH)

    def send_line(k, _):
        line_copy(gx + k).start()
        return 0

    lax.fori_loop(1, ngx - gx, send_line, 0)

    def take_line(h, total):
        line_arrival(h).wait_recv()
        return total + slabs[h]

    energy[...] = lax.fori_loop(0, gx, take_line, mine)[:steps, :own]

    def end_out(x, _):
        pltpu.make_async_copy(psi.at[:, x], psi_out.at[:, x], out_sem.at[x]).wait()
        return 0

    lax.fori_loop(0, cx, end_out, 0)

    for side in range(2):
        for dy in (0, -1, 1):
            @pl.when(jnp.logical_and(sends[0][side], near[dy]))
            def _(side=side, dy=dy):
                z_copy(side, dy).wait_send()

        @pl.when(sends[1][side])
        def _(side=side):
            y_copy(side).wait_send()

        @pl.when(sends[2][side])
        def _(side=side):
            x_copy(side).wait_send()

    def end_one(k, _):
        bin_copy(k).wait_send()
        return 0

    lax.fori_loop(1, peers, end_one, 0)

    def end_line(k, _):
        line_copy(gx + k).wait_send()
        return 0

    lax.fori_loop(1, ngx - gx, end_line, 0)


def body(strain, cell_shell_index, onset_step):
    comps, steps, cx, cy, cz = strain.shape
    shells = onset_step.shape[0]
    ngx, ngy, ngz = lax.axis_size("gx"), lax.axis_size("gy"), lax.axis_size("gz")
    peers = ngy * ngz
    own = shells // peers
    fields = comps * steps
    n_lo = shells // HI
    f32 = jnp.float32
    dma = pltpu.SemaphoreType.DMA
    sizes = (ngx, ngy, ngz, steps, cx, cy, cz, shells)
    anywhere = pl.BlockSpec(memory_space=pltpu.HBM)
    vmem = pl.BlockSpec(memory_space=pltpu.VMEM)
    psi, energy = pl.pallas_call(
        functools.partial(step, sizes),
        out_shape=(
            jax.ShapeDtypeStruct((fields, cx, cy, cz), f32),
            jax.ShapeDtypeStruct((steps, own), f32),
        ),
        in_specs=[anywhere, anywhere, vmem],
        out_specs=(anywhere, vmem),
        scratch_shapes=[
            pltpu.VMEM((fields, cx + 4, cy + 16, cz), f32),
            pltpu.VMEM((cx, cy, cz), jnp.int32),
            pltpu.VMEM((fields, cx, cy, cz), f32),
            pltpu.VMEM((fields, 8, cz), f32),
            pltpu.VMEM((2, fields, 8, cz), f32),
            pltpu.VMEM((fields, 8, cz), f32),
            pltpu.VMEM((2, 8, cz), f32),
            pltpu.VMEM((2, 2, 8, cz), f32),
            pltpu.VMEM((fields * 2 * cx + 8, cz), f32),
            pltpu.VMEM((fields * 2 * cx + 8, cz), f32),
            pltpu.VMEM((2, fields * 2 * cx, cz), f32),
            pltpu.VMEM((fields * 2 * cx + 8, cz), f32),
            pltpu.VMEM((fields * 2 * cx + 8, cz), f32),
            pltpu.VMEM((fields, cy + 16, cz), f32),
            pltpu.VMEM((2 * steps, cy, cz), f32),
            pltpu.VMEM((2 * steps * HI, n_lo), f32),
            pltpu.VMEM((HI, 8, 128), f32),
            pltpu.VMEM((peers, 8, 128), f32),
            pltpu.VMEM((8, 128), f32),
            pltpu.VMEM((ngx, 8, 128), f32),
            dma((2,)), dma((cx,)),
            dma((2,)), dma((2,)), dma((2,)), dma((2,)), dma((2, 3)), dma((2, 3)),
            dma((peers,)), dma((peers,)), dma((ngx,)), dma((ngx,)),
        ],
        compiler_params=pltpu.CompilerParams(
            collective_id=0, has_side_effects=True, vmem_limit_bytes=67043328 - 512 * 1024),
    )(strain.reshape(fields, cx, cy, cz), cell_shell_index, onset_step.reshape(1, shells))
    return psi.reshape(strain.shape), energy[None]


def solution(mesh):
    placed = (P(None, None, "gx", "gy", "gz"), P("gx", "gy", "gz"), P())
    return jax.shard_map(
        body,
        mesh=mesh,
        in_specs=placed,
        out_specs=(P(None, None, "gx", "gy", "gz"), P("gx", None, ("gy", "gz"))),
        check_vma=False,
    )
```

```python
import functools

import jax
import jax.numpy as jnp
from jax import lax
from jax.experimental import pallas as pl
from jax.experimental.pallas import tpu as pltpu
from jax.sharding import PartitionSpec as P

MESH = pl.DeviceIdType.MESH
HI = 8


def step(sizes, strain, cells, onset, psi_out, energy, grid, index, psi, edges, ends, halo_z, corners, corner_in, slope_low, slope_high,
         rows_out, rows_low, rows_high, first_z, some, parts, acc, table, inbox, carry, slabs,
         load_sem, out_sem, send_x, recv_x, send_y, recv_y, send_z, recv_z,
         send_bin, recv_bin, send_acc, recv_acc):
    ngx, ngy, ngz, steps, cx, cy, cz, shells = sizes
    fields = 2 * steps
    n_lo = shells // HI
    peers = ngy * ngz
    own = shells // peers
    gx, gy, gz = lax.axis_index("gx"), lax.axis_index("gy"), lax.axis_index("gz")
    rank = gy * ngz + gz

    load = pltpu.make_async_copy(strain, grid.at[:, pl.ds(2, cx), pl.ds(8, cy), :], load_sem.at[0])
    load.start()
    load_index = pltpu.make_async_copy(cells, index, load_sem.at[1])
    load_index.start()

    barrier = pltpu.get_barrier_semaphore()

    def greet_slab(k, _):
        q = lax.rem(rank + k, peers)
        pl.semaphore_signal(barrier, inc=1, device_id=(gx, q // ngz, lax.rem(q, ngz)), device_id_type=MESH)
        return 0

    def greet_line(k, _):
        pl.semaphore_signal(barrier, inc=1, device_id=(lax.rem(gx + k, ngx), gy, gz), device_id_type=MESH)
        return 0

    lax.fori_loop(1, ngx, greet_line, 0)
    lax.fori_loop(1, peers, greet_slab, 0)
    load.wait()

    lane = lax.broadcasted_iota(jnp.int32, (8, cz), 1)
    row = lax.broadcasted_iota(jnp.int32, (8, cz), 0)
    slot_of_lane = lane // 4

    for f in range(fields):
        for x in range(cx):
            rows_out[0, pl.ds(f * 2 * cx + 2 * x, 2), :] = grid[f, x + 2, pl.ds(8, 2), :]
            rows_out[1, pl.ds(f * 2 * cx + 2 * x, 2), :] = grid[f, x + 2, pl.ds(6 + cy, 2), :]

    pl.semaphore_wait(barrier, peers - 1 + ngx - 1)

    def x_copy(side):
        there = gx + 1 if side == 0 else gx - 1
        return pltpu.make_async_remote_copy(
            src_ref=grid.at[:, pl.ds(cx if side == 0 else 2, 2), pl.ds(8, cy), :],
            dst_ref=grid.at[:, pl.ds(0 if side == 0 else cx + 2, 2), pl.ds(8, cy), :],
            send_sem=send_x.at[side], recv_sem=recv_x.at[side],
            device_id=(there, gy, gz), device_id_type=MESH)

    def y_copy(side):
        there = gy + 1 if side == 0 else gy - 1
        return pltpu.make_async_remote_copy(
            src_ref=rows_out.at[1 - side],
            dst_ref=(rows_low.at[pl.ds(8, fields * 2 * cx), :] if side == 0
                     else rows_high.at[pl.ds(0, fields * 2 * cx), :]),
            send_sem=send_y.at[side], recv_sem=recv_y.at[side],
            device_id=(gx, there, gz), device_id_type=MESH)

    def z_copy(side, dy):
        there = gz + 1 if side == 0 else gz - 1
        return pltpu.make_async_remote_copy(
            src_ref=edges if dy == 0 else corners.at[0 if dy < 0 else 1],
            dst_ref=ends.at[side] if dy == 0 else corner_in.at[side, 0 if dy > 0 else 1],
            send_sem=send_z.at[side, 1 - dy], recv_sem=recv_z.at[side, 1 - dy],
            device_id=(gx, gy + dy, there), device_id_type=MESH)

    sends = ([gz < ngz - 1, gz > 0], [gy < ngy - 1, gy > 0], [gx < ngx - 1, gx > 0])
    gets = ([gz > 0, gz < ngz - 1], [gy > 0, gy < ngy - 1], [gx > 0, gx < ngx - 1])
    near = {-1: gy > 0, 0: gy >= 0, 1: gy < ngy - 1}

    for side in range(2):
        @pl.when(sends[1][side])
        def _(side=side):
            y_copy(side).start()

    for f in range(fields):
        packed = jnp.zeros((8, cz), jnp.float32)
        for x in range(cx):
            for half in range(2):
                slot = 2 * x + half
                moved = pltpu.roll(grid[f, x + 2, pl.ds(8 + 8 * half, 8), :], (2 + 4 * slot) % cz, 1)
                packed = jnp.where(slot_of_lane == slot, moved, packed)
        edges[f] = packed
    for side in range(2):
        packed = jnp.zeros((8, cz), jnp.float32)
        for slot in range(fields * cx // 4):
            moved = pltpu.roll(rows_out[side, pl.ds(8 * slot, 8), :], (2 + 4 * slot) % cz, 1)
            packed = jnp.where(slot_of_lane == slot, moved, packed)
        corners[side] = packed

    for side in range(2):
        @pl.when(sends[2][side])
        def _(side=side):
            x_copy(side).start()
    for side in range(2):
        for dy in (0, -1, 1):
            @pl.when(jnp.logical_and(sends[0][side], near[dy]))
            def _(side=side, dy=dy):
                z_copy(side, dy).start()

    for side in range(2):
        for dy in (-1, 0, 1):
            @pl.when(jnp.logical_not(jnp.logical_and(gets[0][side], near[dy])))
            def _(side=side, dy=dy):
                if dy == 0:
                    ends[side] = jnp.zeros(ends.shape[1:], jnp.float32)
                else:
                    corner_in[side, 0 if dy < 0 else 1] = jnp.zeros((8, cz), jnp.float32)

        @pl.when(jnp.logical_not(gets[2][side]))
        def _(side=side):
            grid[:, pl.ds(0 if side == 0 else cx + 2, 2), pl.ds(8, cy), :] = jnp.zeros(
                (fields, 2, cy, cz), jnp.float32)

    @pl.when(jnp.logical_not(gets[1][0]))
    def _():
        rows_low[...] = jnp.zeros(rows_low.shape, jnp.float32)

    @pl.when(jnp.logical_not(gets[1][1]))
    def _():
        rows_high[...] = jnp.zeros(rows_high.shape, jnp.float32)

    acc[...] = jnp.zeros(acc.shape, jnp.float32)
    table[...] = jnp.zeros(table.shape, jnp.float32)
    load_index.wait()

    for side in range(2):
        for dy in (0, -1, 1):
            @pl.when(jnp.logical_and(gets[0][side], near[dy]))
            def _(side=side, dy=dy):
                z_copy(side, -dy).wait_recv()

    from_left = lax.rem(lane, 4) < 2
    for f in range(fields):
        halo_z[f] = jnp.where(from_left, ends[0, f], ends[1, f])

    wide = lax.broadcasted_iota(jnp.int32, (cy, cz), 0)
    far = lax.broadcasted_iota(jnp.int32, (cy, cz), 1)
    uy = ((gy * cy + wide).astype(jnp.float32) + 0.5) / (cy * ngy) - 0.5
    uz = ((gz * cz + far).astype(jnp.float32) + 0.5) / (cz * ngz) - 0.5
    rsq_yz = uy * uy + uz * uz + 0.05
    low_label = lax.broadcasted_iota(jnp.int32, (n_lo, cz), 0)
    head, tail = lane < 2, lane >= cz - 2

    def along(cell, halo, shift):
        ring = pltpu.roll(halo, shift, 1)
        m2 = pltpu.roll(jnp.where(tail, ring, cell), 2, 1)
        m1 = pltpu.roll(jnp.where(lane == cz - 1, ring, cell), 1, 1)
        p1 = pltpu.roll(jnp.where(lane == 0, ring, cell), cz - 1, 1)
        p2 = pltpu.roll(jnp.where(head, ring, cell), cz - 2, 1)
        return m2, m1, p1, p2

    def z_part(i, _):
        for u in range(2):
            x = 2 * i + u
            for f in range(fields):
                for half in range(2):
                    at = pl.ds(8 + 8 * half, 8)
                    cell = grid[f, x + 2, at, :]
                    m2, m1, p1, p2 = along(cell, halo_z[f], lax.rem(2 * cz - 2 - 4 * half - 8 * x, cz))
                    first_z[f, x, at, :] = 8.0 * (p1 - m1) - (p2 - m2)
                    some[f, x, pl.ds(8 * half, 8), :] = (p2 + m2) - 16.0 * (p1 + m1) - 30.0 * cell
        return 0

    lax.fori_loop(0, cx // 2, z_part, 0)

    for side in range(2):
        @pl.when(gets[1][side])
        def _(side=side):
            y_copy(side).wait_recv()

    for end, (rows, first, slope) in enumerate(((rows_low, 8, slope_low), (rows_high, 0, slope_high))):
        @pl.when(gets[1][end])
        def _(end=end, rows=rows, first=first, slope=slope):
            ring = jnp.where(from_left, corner_in[0, end], corner_in[1, end])
            for slot in range(fields * cx // 4):
                m2, m1, p1, p2 = along(rows[pl.ds(first + 8 * slot, 8), :], ring, (2 * cz - 2 - 4 * slot) % cz)
                slope[pl.ds(first + 8 * slot, 8), :] = 8.0 * (p1 - m1) - (p2 - m2)

        @pl.when(jnp.logical_not(gets[1][end]))
        def _(slope=slope):
            slope[...] = jnp.zeros(slope.shape, jnp.float32)


    def outer_rows(x, _):
        for f in range(fields):
            base = f * 2 * cx + 2 * x
            outside = jnp.where(row < 4, rows_high[pl.ds(base, 8), :], rows_low[pl.ds(base + 2, 8), :])
            d = jnp.where(row < 4, slope_high[pl.ds(base, 8), :], slope_low[pl.ds(base + 2, 8), :])
            grid[f, x + 2, pl.ds(0, 8), :] = outside
            grid[f, x + 2, pl.ds(8 + cy, 8), :] = outside
            first_z[f, x, pl.ds(0, 8), :] = d
            first_z[f, x, pl.ds(8 + cy, 8), :] = d
        return 0

    lax.fori_loop(0, cx, outer_rows, 0)

    def stencil(x, u):
        combo, mixed = [], []
        for f in range(fields):
            near_xy = (grid[f, x + 1, pl.ds(8, cy), :] + grid[f, x + 3, pl.ds(8, cy), :]
                       + grid[f, x + 2, pl.ds(7, cy), :] + grid[f, x + 2, pl.ds(9, cy), :])
            far_xy = (grid[f, x, pl.ds(8, cy), :] + grid[f, x + 4, pl.ds(8, cy), :]
                      + grid[f, x + 2, pl.ds(6, cy), :] + grid[f, x + 2, pl.ds(10, cy), :])
            combo.append(16.0 * near_xy - far_xy + some[f, x])
            mixed.append(8.0 * (first_z[f, x, pl.ds(9, cy), :] - first_z[f, x, pl.ds(7, cy), :])
                         - (first_z[f, x, pl.ds(10, cy), :] - first_z[f, x, pl.ds(6, cy), :]))
        ux = ((gx * cx + x).astype(jnp.float32) + 0.5) * (1.0 / (cx * ngx)) - 0.5
        rsq = (rsq_yz + ux * ux) * 0.0625
        news_re = jnp.zeros((cy, cz), jnp.float32)
        news_im = jnp.zeros((cy, cz), jnp.float32)
        for t in range(steps):
            re = combo[t] * (1.0 / 24.0) - mixed[steps + t] * (1.0 / 144.0)
            im = combo[steps + t] * (-1.0 / 24.0) - mixed[t] * (1.0 / 144.0)
            psi[t, x] = re
            psi[steps + t, x] = im
            news_re, news_im = news_re + re, news_im + im
            flux = rsq * (news_re * news_re + news_im * news_im)
            coarse = flux.astype(jnp.bfloat16).astype(jnp.float32)
            parts[u, 2 * t] = coarse
            parts[u, 2 * t + 1] = flux - coarse

    def bins(x, u, total):
        group = 4
        for y0 in range(0, cy, group):
            left, right = [], []
            hit = []
            for y in range(y0, y0 + group):
                shell = index[x, pl.ds(y, 1), :]
                high = shell // n_lo
                low = shell - high * n_lo
                hit.append(jnp.broadcast_to(high, (HI, cz)) == row)
                right.append(jnp.where(jnp.broadcast_to(low, (n_lo, cz)) == low_label, 1.0, 0.0))
            for p in range(2 * steps):
                left.append(jnp.concatenate(
                    [jnp.where(hit[k], jnp.broadcast_to(parts[u, p, pl.ds(y0 + k, 1), :], (HI, cz)), 0.0)
                     for k in range(group)], 1))
            total = total + lax.dot_general(
                jnp.concatenate(left, 0).astype(jnp.bfloat16),
                jnp.concatenate(right, 1).astype(jnp.bfloat16),
                (((1,), (1,)), ((), ())), preferred_element_type=jnp.float32)
        return total

    def pair(i, _):
        @pl.when(i == cx // 2 - 2)
        def _():
            for side in range(2):
                @pl.when(gets[2][side])
                def _(side=side):
                    x_copy(side).wait_recv()

        first = lax.rem(2 * i + 2, cx)
        for u in range(2):
            stencil(first + u, u)
        pltpu.make_async_copy(psi.at[:, pl.ds(first, 2)], psi_out.at[:, pl.ds(first, 2)], out_sem.at[i]).start()
        total = acc[...]
        for u in range(2):
            total = bins(first + u, u, total)
        acc[...] = total
        return 0

    lax.fori_loop(0, cx // 2, pair, 0)

    for t in range(steps):
        both = acc[pl.ds(16 * t, 8), :] + acc[pl.ds(16 * t + 8, 8), :]
        for h in range(HI):
            table[h, pl.ds(t, 1), pl.ds(0, n_lo)] = both[h:h + 1, :]

    spread = peers // HI

    def bin_copy(k):
        q = lax.rem(rank + k, peers)
        return pltpu.make_async_remote_copy(
            src_ref=table.at[q // spread], dst_ref=inbox.at[rank],
            send_sem=send_bin.at[k], recv_sem=recv_bin.at[rank],
            device_id=(gx, q // ngz, lax.rem(q, ngz)), device_id_type=MESH)

    def bin_arrival(k):
        q = lax.rem(rank + k, peers)
        return pltpu.make_async_remote_copy(
            src_ref=table.at[0], dst_ref=inbox.at[q],
            send_sem=send_bin.at[k], recv_sem=recv_bin.at[q],
            device_id=(gx, q // ngz, lax.rem(q, ngz)), device_id_type=MESH)

    def send_one(k, _):
        bin_copy(k).start()
        return 0

    lax.fori_loop(1, peers, send_one, 0)

    def take_one(k, total):
        bin_arrival(k).wait_recv()
        return total + inbox[lax.rem(rank + k, peers)]

    total = lax.fori_loop(1, peers, take_one, table[rank // spread])
    first = rank * own
    labels = jnp.zeros((8, 128), jnp.int32)
    for block in range(shells // 128):
        piece = jnp.broadcast_to(onset[:, pl.ds(block * 128, 128)], (8, 128))
        labels = jnp.where(first // 128 == block, piece, labels)
    labels = pltpu.roll(labels, lax.rem(128 - lax.rem(first, 128), 128), 1)
    total = pltpu.roll(total, lax.rem(128 - lax.rem(rank, spread) * own, 128), 1)
    total = jnp.where(row >= labels, total, 0.0)
    scale = 0.25 * shells / (cx * ngx * cy * ngy * cz * ngz)
    running = jnp.zeros((1, 128), jnp.float32)
    sums = []
    for t in range(steps):
        running = running + total[t:t + 1, :]
        sums.append(running * scale)
    sums.append(jnp.zeros((8 - steps, 128), jnp.float32))
    mine = jnp.concatenate(sums, 0)
    carry[...] = mine

    def line_copy(there):
        return pltpu.make_async_remote_copy(
            src_ref=carry, dst_ref=slabs.at[gx],
            send_sem=send_acc.at[there], recv_sem=recv_acc.at[gx],
            device_id=(there, gy, gz), device_id_type=MESH)

    def line_arrival(h):
        return pltpu.make_async_remote_copy(
            src_ref=carry, dst_ref=slabs.at[h],
            send_sem=send_acc.at[h], recv_sem=recv_acc.at[h],
            device_id=(h, gy, gz), device_id_type=MESH)

    def send_line(k, _):
        line_copy(gx + k).start()
        return 0

    lax.fori_loop(1, ngx - gx, send_line, 0)

    def take_line(h, total):
        line_arrival(h).wait_recv()
        return total + slabs[h]

    energy[...] = lax.fori_loop(0, gx, take_line, mine)[:steps, :own]

    def end_out(i, _):
        first = lax.rem(2 * i + 2, cx)
        pltpu.make_async_copy(psi.at[:, pl.ds(first, 2)], psi_out.at[:, pl.ds(first, 2)], out_sem.at[i]).wait()
        return 0

    lax.fori_loop(0, cx // 2, end_out, 0)

    for side in range(2):
        for dy in (0, -1, 1):
            @pl.when(jnp.logical_and(sends[0][side], near[dy]))
            def _(side=side, dy=dy):
                z_copy(side, dy).wait_send()

        @pl.when(sends[1][side])
        def _(side=side):
            y_copy(side).wait_send()

        @pl.when(sends[2][side])
        def _(side=side):
            x_copy(side).wait_send()

    def end_one(k, _):
        bin_copy(k).wait_send()
        return 0

    lax.fori_loop(1, peers, end_one, 0)

    def end_line(k, _):
        line_copy(gx + k).wait_send()
        return 0

    lax.fori_loop(1, ngx - gx, end_line, 0)


def body(strain, cell_shell_index, onset_step):
    comps, steps, cx, cy, cz = strain.shape
    shells = onset_step.shape[0]
    ngx, ngy, ngz = lax.axis_size("gx"), lax.axis_size("gy"), lax.axis_size("gz")
    peers = ngy * ngz
    own = shells // peers
    fields = comps * steps
    n_lo = shells // HI
    f32 = jnp.float32
    dma = pltpu.SemaphoreType.DMA
    sizes = (ngx, ngy, ngz, steps, cx, cy, cz, shells)
    anywhere = pl.BlockSpec(memory_space=pltpu.HBM)
    vmem = pl.BlockSpec(memory_space=pltpu.VMEM)
    psi, energy = pl.pallas_call(
        functools.partial(step, sizes),
        out_shape=(
            jax.ShapeDtypeStruct((fields, cx, cy, cz), f32),
            jax.ShapeDtypeStruct((steps, own), f32),
        ),
        in_specs=[anywhere, anywhere, vmem],
        out_specs=(anywhere, vmem),
        scratch_shapes=[
            pltpu.VMEM((fields, cx + 4, cy + 16, cz), f32),
            pltpu.VMEM((cx, cy, cz), jnp.int32),
            pltpu.VMEM((fields, cx, cy, cz), f32),
            pltpu.VMEM((fields, 8, cz), f32),
            pltpu.VMEM((2, fields, 8, cz), f32),
            pltpu.VMEM((fields, 8, cz), f32),
            pltpu.VMEM((2, 8, cz), f32),
            pltpu.VMEM((2, 2, 8, cz), f32),
            pltpu.VMEM((fields * 2 * cx + 8, cz), f32),
            pltpu.VMEM((fields * 2 * cx + 8, cz), f32),
            pltpu.VMEM((2, fields * 2 * cx, cz), f32),
            pltpu.VMEM((fields * 2 * cx + 8, cz), f32),
            pltpu.VMEM((fields * 2 * cx + 8, cz), f32),
            pltpu.VMEM((fields, cx, cy + 16, cz), f32),
            pltpu.VMEM((fields, cx, cy, cz), f32),
            pltpu.VMEM((2, 2 * steps, cy, cz), f32),
            pltpu.VMEM((2 * steps * HI, n_lo), f32),
            pltpu.VMEM((HI, 8, 128), f32),
            pltpu.VMEM((peers, 8, 128), f32),
            pltpu.VMEM((8, 128), f32),
            pltpu.VMEM((ngx, 8, 128), f32),
            dma((2,)), dma((cx // 2,)),
            dma((2,)), dma((2,)), dma((2,)), dma((2,)), dma((2, 3)), dma((2, 3)),
            dma((peers,)), dma((peers,)), dma((ngx,)), dma((ngx,)),
        ],
        compiler_params=pltpu.CompilerParams(
            collective_id=0, has_side_effects=True, vmem_limit_bytes=67043328 - 512 * 1024),
    )(strain.reshape(fields, cx, cy, cz), cell_shell_index, onset_step.reshape(1, shells))
    return psi.reshape(strain.shape), energy[None]


def solution(mesh):
    placed = (P(None, None, "gx", "gy", "gz"), P("gx", "gy", "gz"), P())
    return jax.shard_map(
        body,
        mesh=mesh,
        in_specs=placed,
        out_specs=(P(None, None, "gx", "gy", "gz"), P("gx", None, ("gy", "gz"))),
        check_vma=False,
    )
```
